32 devices in a mesh: ep: 16 (over z, y, x), half: 2 (over core).
Axes of the slice: x: 2, y: 2, z: 4, core: 2. Of those that a mesh axis runs over, the one named last changes fastest.
Arguments:
- tokens: bfloat16 [2048, 2048], P('ep', 'half'), may hold values from -6 to 6
- gate_weights: float32 [2048, 8], P('ep'), may hold values from 0.05 to 0.3
- expert_ids: int32 [2048, 8], P('ep'), may hold values from 0 to 15, all different within a row; in each aligned block of 128 rows (0 to 127, 128 to 255, ...) at most 80 rows name the same one
- w_gate: bfloat16 [16, 2048, 768], P('ep', None, 'half'), may hold values from -0.125 to 0.125
- w_up: bfloat16 [16, 2048, 768], P('ep', None, 'half'), may hold values from -0.125 to 0.125
- w_down: bfloat16 [16, 768, 2048], P('ep', 'half'), may hold values from -0.21875 to 0.21875
Outputs:
- mixed: bfloat16 [2048, 2048], P('ep', 'half')
The draws below stay inside these ranges and needn't reach their ends.
Inputs may be any that keep to these rules, and one draw needn't show every extreme that they name: `expert_ids`: each row names 8 different experts. Within the rows of one device (aligned blocks of 128 rows) no expert is named by more than 80 rows, and in every draw some expert is named by exactly 80 rows of some block.
All inputs are finite; a program needn't handle non-finite values.
Results may differ from the reference program's by a relative error of at most 0.0085.
Values may be sent and summed in bfloat16 or wider, within the bound.
A program may use at most 64 MiB of HBM per device.

```python
import math
import jax
import jax.numpy as jnp
import numpy as np
from jax import lax

D = 2048
FF = 768
TOP = 8
TOK_DEV = 128
EXPERTS = 16
TOKENS = 2048
CAP = 80
N_EP = 16


def steps_of(own_key, shape, shards, low, largest):
    factor_of = 1.0
    for axis_at, shards_of in shards:
        steps = jax.random.uniform(jax.random.fold_in(jax.random.fold_in(own_key, 6), axis_at), (shards_of,), jnp.float32, low / len(shards), largest / len(shards))
        factor_of = factor_of * jnp.repeat(jnp.exp(steps), shape[axis_at] // shards_of).reshape((-1,) + (1,) * (len(shape) - 1 - axis_at))
    return factor_of


def deal_out(rng, own, number, rows, amount, top, reach, slope):
    sequence = jax.random.permutation(rng, amount)
    crowded, common = shares(amount, rows * top, reach, slope, True), shares(amount, rows * top, reach, slope, False)
    places = jnp.arange(amount)

    def named(lengths, rotation):
        used = int((lengths > 0).sum())
        fixed = max(1, used // 4)
        passed = fixed + (places - fixed + rotation * (used - fixed)) % max(1, amount - fixed)
        return jnp.zeros((amount,), jnp.int32).at[sequence[jnp.where(places < fixed, places, passed)]].set(jnp.asarray(lengths, jnp.int32))

    lengths = jnp.where(number % 4 == 0, named(crowded, number // 4), named(common, number - number // 4 - 1))
    mixed = jax.random.permutation(jax.random.fold_in(own, 3), amount)
    giver, receiver = mixed[0:amount // 2 * 2:2], mixed[1:amount // 2 * 2:2]
    margin = jnp.minimum(lengths[giver] - 1, reach - lengths[receiver]) // 2
    margin = jnp.where((giver == sequence[0]) | (receiver == sequence[0]) | (lengths[receiver] == 0), 0, jnp.maximum(margin, 0))
    passed = jax.random.randint(jax.random.fold_in(own, 4), (amount // 2,), 0, 1 << 20) % (margin + 1)
    lengths = lengths.at[giver].add(-passed).at[receiver].add(passed)
    items = jnp.searchsorted(jnp.cumsum(lengths), jnp.arange(rows * top), side="right").astype(jnp.int32)
    table = items.reshape(top, rows).T
    table = table[jax.random.permutation(jax.random.fold_in(own, 1), rows)]
    rotation = jax.random.randint(jax.random.fold_in(own, 2), (rows, 1), 0, top)
    return jnp.take_along_axis(table, (jnp.arange(top)[None, :] + rotation) % top, axis=1)


def shares(amount, total, limit, lean, full):
    weights = [(1 << 20) // math.isqrt(rank ** lean) + 1 for rank in range(1, amount + 1)]
    largest = limit if full else min(limit, max(-(-total // amount), total * weights[0] // sum(weights)))
    least = 1 if total - largest >= amount - 1 else 0
    holding, rest = [largest] + [least] * (amount - 1), total - largest - least * (amount - 1)
    while rest > 0:
        candidates = [i for i in range(1, amount) if holding[i] < largest] or [i for i in range(1, amount) if holding[i] < limit]
        pool, remaining = sum([weights[i] for i in candidates]), rest
        for i in candidates:
            more = min(limit - holding[i], max(1, remaining * weights[i] // pool), rest)
            holding[i] = holding[i] + more
            rest = rest - more
    return np.array(holding)


def scatter_about(key, extent, deviation, reach, shards=(), kind=jnp.bfloat16):
    entries = jax.random.normal(key, extent, jnp.float32) * deviation
    if len(shards) > 0:
        entries = steps_of(key, extent, shards, -0.22, 0.18) * entries
    return jnp.clip(entries, min=-reach, max=reach).astype(kind)


def setup_inputs(seed: int = 0) -> dict:
    arg_keys = jax.random.split(jax.random.key(seed), 7)
    tokens = scatter_about(arg_keys[0], (TOKENS, D), 1.0, 6.0, ((0, 16), (1, 2)))
    gate_weights = jnp.clip(0.05 + 0.25 * jax.random.uniform(arg_keys[1], (TOKENS, TOP), jnp.float32) ** steps_of(arg_keys[1], (TOKENS, TOP), ((0, 16),), -0.2, 0.2), 0.05, 0.3)
    expert_ids_keys = jax.random.split(jax.random.fold_in(arg_keys[2], 1), TOKENS // TOK_DEV)
    expert_ids_turns = jax.random.permutation(jax.random.fold_in(arg_keys[2], 3), TOKENS // TOK_DEV)
    expert_ids = jax.vmap(lambda own, number: deal_out(jax.random.fold_in(arg_keys[2], 2), own, number, TOK_DEV, EXPERTS, TOP, CAP, 2))(expert_ids_keys, expert_ids_turns).reshape((TOKENS, TOP))
    w_gate = scatter_about(arg_keys[3], (EXPERTS, D, FF), D ** -0.5, 0.125, ((0, 16), (2, 2)))
    w_up = scatter_about(arg_keys[4], (EXPERTS, D, FF), D ** -0.5, 0.125, ((0, 16), (2, 2)))
    w_down = scatter_about(arg_keys[5], (EXPERTS, FF, D), FF ** -0.5, 0.21875, ((0, 16), (1, 2)))
    return {"tokens": tokens, "gate_weights": gate_weights, "expert_ids": expert_ids, "w_gate": w_gate, "w_up": w_up, "w_down": w_down}


def rank_block(block):
    columns = jnp.arange(EXPERTS, dtype=jnp.int32)
    onehot = (block[:, None] == columns[None, :]).astype(jnp.int32)
    before = jnp.cumsum(onehot, axis=0) - onehot
    return jnp.sum(before * onehot, axis=1).astype(jnp.int32)


def reference(tokens, gate_weights, expert_ids, w_gate, w_up, w_down):
    ids = expert_ids.reshape(N_EP, TOK_DEV * TOP).astype(jnp.int32)
    ranks = lax.map(rank_block, ids)
    slot = (ids * CAP + ranks).astype(jnp.int32)
    source = jnp.arange(N_EP, dtype=jnp.int32)[:, None]
    local_token = (jnp.arange(TOK_DEV * TOP, dtype=jnp.int32) // TOP)[None, :]
    token_table = jnp.zeros((N_EP, EXPERTS * CAP), jnp.int32).at[source, slot].set(source * TOK_DEV + local_token)
    weight_table = jnp.zeros((N_EP, EXPERTS * CAP), jnp.float32).at[source, slot].set(gate_weights.reshape(N_EP, TOK_DEV * TOP))
    filled = jnp.zeros((N_EP, EXPERTS * CAP), jnp.bfloat16).at[source, slot].set(jnp.ones((N_EP, TOK_DEV * TOP), jnp.bfloat16))
    token_table = token_table.reshape(N_EP, EXPERTS, CAP).transpose(1, 0, 2).reshape(EXPERTS, N_EP * CAP)
    weight_table = weight_table.reshape(N_EP, EXPERTS, CAP).transpose(1, 0, 2).reshape(EXPERTS, N_EP * CAP)
    filled = filled.reshape(N_EP, EXPERTS, CAP).transpose(1, 0, 2).reshape(EXPERTS, N_EP * CAP)
    middle = FF // 2

    def expert_step(total, inputs):
        gate_mat, up_mat, down_mat, rows, weights, used = inputs
        slot_rows = tokens[rows] * used[:, None]
        gate = jnp.dot(slot_rows, gate_mat, preferred_element_type=jnp.float32)
        up = jnp.dot(slot_rows, up_mat, preferred_element_type=jnp.float32)
        hidden = (jax.nn.silu(gate) * up).astype(jnp.bfloat16)
        first = jnp.dot(hidden[:, :middle], down_mat[:middle], preferred_element_type=jnp.float32)
        second = jnp.dot(hidden[:, middle:], down_mat[middle:], preferred_element_type=jnp.float32)
        first = lax.optimization_barrier(first.astype(jnp.bfloat16)).astype(jnp.float32)
        second = lax.optimization_barrier(second.astype(jnp.bfloat16)).astype(jnp.float32)
        expert_out = lax.optimization_barrier((first + second).astype(jnp.bfloat16)).astype(jnp.float32)
        total = total.at[rows].add(weights[:, None] * expert_out)
        return total, None

    start = jnp.zeros((TOKENS, D), jnp.float32)
    total, unused = lax.scan(expert_step, start, (w_gate, w_up, w_down, token_table, weight_table, filled))
    return total.astype(jnp.bfloat16)
```

```python
import functools

import jax
import jax.numpy as jnp
from jax import lax
from jax.experimental import pallas as pl
from jax.experimental.pallas import tpu as pltpu
from jax.sharding import PartitionSpec as P

MESH = pl.DeviceIdType.MESH


def slots(tokens, gate_weights, expert_ids, w_gate, w_up, w_down):
    tok_dev, half_width = tokens.shape
    top = expert_ids.shape[1]
    local_experts = w_gate.shape[0]
    experts = local_experts * lax.axis_size("ep")
    capacity = min(tok_dev, max(2, 5 * tok_dev * top // (4 * experts)))
    flat_ids = expert_ids.reshape(-1)
    columns = jnp.arange(experts, dtype=jnp.int32)
    onehot = (flat_ids[:, None] == columns[None, :]).astype(jnp.int32)
    ranks = jnp.sum((jnp.cumsum(onehot, axis=0) - onehot) * onehot, axis=1)
    slot = flat_ids * capacity + ranks
    token_of_pair = jnp.arange(tok_dev * top, dtype=jnp.int32) // top
    token_table = jnp.zeros((experts * capacity,), jnp.int32).at[slot].set(token_of_pair)
    filled = (
        jnp.zeros((experts * capacity,), jnp.bfloat16)
        .at[slot]
        .set(jnp.ones((tok_dev * top,), jnp.bfloat16))
    )
    outgoing = (tokens[token_table] * filled[:, None]).reshape(experts, capacity, half_width)
    received = lax.all_to_all(outgoing, "ep", split_axis=0, concat_axis=0, tiled=True)
    count = received.shape[1]
    whole = lax.all_gather(received, "half", axis=2, tiled=True)
    width = whole.shape[2]
    grouped = whole.reshape(-1, local_experts, count, width)
    gate = jnp.einsum("secd,edf->secf", grouped, w_gate, preferred_element_type=jnp.float32)
    up = jnp.einsum("secd,edf->secf", grouped, w_up, preferred_element_type=jnp.float32)
    hidden = (jax.nn.silu(gate) * up).astype(jnp.bfloat16)
    partial_out = jnp.einsum("secf,efd->secd", hidden, w_down, preferred_element_type=jnp.float32)
    partial_out = partial_out.astype(jnp.bfloat16).reshape(experts, count, width)
    widened = lax.optimization_barrier(partial_out).astype(jnp.float32)
    summed = lax.psum_scatter(widened.astype(jnp.bfloat16), "half", scatter_dimension=2, tiled=True)
    answer = lax.all_to_all(summed, "ep", split_axis=0, concat_axis=0, tiled=True)
    picked = answer.reshape(experts * capacity, -1)[slot].reshape(tok_dev, top, -1)
    slot_out = picked.astype(jnp.float32)
    mixed = jnp.einsum("tk,tkx->tx", gate_weights, slot_out)
    return mixed.astype(jnp.bfloat16)


def kernel(nz, tok_ref, gw_ref, ids_ref, wg_ref, wu_ref, wd_ref, out_ref,
           xg, wgu, wdn, pa, pb, da, db, rxa, rxb, rya, ryb, own, zs, rz, fin, rfin,
           load_sem, pre_sem, wsend, wrecv, zsend, zrecv, xsend, xrecv, ysend, yrecv,
           fxsend, fxrecv, fysend, fyrecv,
           esend, erecv, dsend, drecv, csend, crecv, qsend, qrecv, fsend, frecv):
    ep = lax.axis_index("ep")
    core = lax.axis_index("half")
    x, y, z = ep % 2, (ep // 2) % 2, ep // 4
    rows, width = out_ref.shape[0] // 2, wg_ref.shape[1]
    half, ff = width // 2, wg_ref.shape[2]
    other = {"half": 1 - core}
    xn = {"ep": z * 4 + y * 2 + (1 - x)}
    yn = {"ep": z * 4 + (1 - y) * 2 + x}

    def zn(to):
        return {"ep": to * 4 + y * 2 + x}

    def send(src, dst, s, r, to):
        return pltpu.make_async_remote_copy(
            src_ref=src, dst_ref=dst, send_sem=s, recv_sem=r, device_id=to, device_id_type=MESH
        )

    def at(d):
        return (z + nz - d) % nz

    loads = [
        pltpu.make_async_copy(wg_ref.at[0], wgu.at[0, :, pl.ds(0, ff)], load_sem.at[0]),
        pltpu.make_async_copy(wu_ref.at[0], wgu.at[0, :, pl.ds(ff, ff)], load_sem.at[1]),
        pltpu.make_async_copy(wd_ref.at[0], wdn.at[pl.ds(0, ff)], load_sem.at[2]),
    ]
    mine = pltpu.make_async_copy(
        tok_ref.at[pl.ds(core * rows, rows)],
        xg.at[0, z, :, pl.ds(pl.multiple_of(core * half, 128), half)],
        load_sem.at[3],
    )
    mine.start()
    for load in loads:
        load.start()

    lane = lax.broadcasted_iota(jnp.int32, (rows, 128), 1)
    spread = jnp.zeros((rows, 128), jnp.float32)
    ids = ids_ref[pl.ds(core * rows, rows), :]
    weights = gw_ref[pl.ds(core * rows, rows), :]
    for k in range(ids.shape[1]):
        spread += jnp.where(lane % 64 == ids[:, k : k + 1], weights[:, k : k + 1], 0.0)
    upper = spread.astype(jnp.bfloat16).astype(jnp.float32)
    both = jnp.where(lane < 64, upper, spread - upper)
    xg[0, z, :, width : width + 128] = both.astype(jnp.bfloat16)

    barrier = pltpu.get_barrier_semaphore()
    partners = [other, xn, yn] + [zn(at(d)) for d in range(1, nz)]
    for partner in partners:
        pl.semaphore_signal(barrier, inc=1, device_id=partner, device_id_type=MESH)
    pl.semaphore_wait(barrier, len(partners))

    pre = send(
        tok_ref.at[pl.ds((1 - core) * rows, rows)],
        xg.at[0, z, :, pl.ds(pl.multiple_of(core * half, 128), half)],
        pre_sem.at[0], pre_sem.at[1], other,
    )
    pre.start()
    swaps = [
        send(wg_ref.at[0], wgu.at[1, :, pl.ds(0, ff)], wsend.at[0], wrecv.at[0], other),
        send(wu_ref.at[0], wgu.at[1, :, pl.ds(ff, ff)], wsend.at[1], wrecv.at[1], other),
        send(wd_ref.at[0], wdn.at[pl.ds(ff, ff)], wsend.at[2], wrecv.at[2], other),
    ]
    mine.wait()
    pre.wait_recv()
    sent = [pre]

    def go(copy):
        copy.start()
        sent.append(copy)
        return copy

    first, last = pl.ds(0, half), pl.ds(half, half + 128)
    xs, ys, fx, fy, zc = {}, {}, {}, {}, {}

    def column(d):
        b = xg.at[0, at(d)]
        xs[d] = go(send(b, xg.at[1, at(d)], xsend.at[d], xrecv.at[d], xn))
        ys[d] = go(send(b, xg.at[2, at(d)], ysend.at[d], yrecv.at[d], yn))

    def forward(d):
        ys[d].wait_recv()
        fx[d] = go(send(xg.at[2, at(d), :, last], xg.at[3, at(d), :, last],
                        fxsend.at[d], fxrecv.at[d], xn))
        xs[d].wait_recv()
        fy[d] = go(send(xg.at[1, at(d), :, first], xg.at[3, at(d), :, first],
                        fysend.at[d], fyrecv.at[d], yn))

    for d in range(1, nz):
        zc[d] = go(send(xg.at[0, z], xg.at[0, z], zsend.at[d - 1], zrecv.at[d - 1], zn((z + d) % nz)))
    column(0)
    for swap in swaps:
        go(swap)
    for d in range(1, nz):
        zc[d].wait_recv()
        column(d)
        forward(d - 1)

    many = nz * rows

    def expert(g):
        lanes = lax.broadcasted_iota(jnp.int32, (many, 128), 1)
        table = xg[g, :, :, width : width + 128].reshape(many, 128).astype(jnp.float32)
        weight = jnp.sum(jnp.where(lanes % 64 == ep, table, 0.0), axis=1, keepdims=True)
        rows_in = xg[g, :, :, 0:width].reshape(many, width)
        parts = []
        for side in range(2):
            gu = jnp.dot(rows_in, wgu[side], preferred_element_type=jnp.float32)
            gate, up = gu[:, :ff], gu[:, ff:]
            hid = gate / (1.0 + jnp.exp(-gate)) * up * weight
            parts.append(hid.astype(jnp.bfloat16))
        hidden = jnp.concatenate(parts, axis=1)
        for to, start in ((pa, 0), (pb, half)):
            o = jnp.dot(hidden, wdn[:, start : start + half], preferred_element_type=jnp.float32)
            to[g] = o.astype(jnp.bfloat16).reshape(nz, rows, half)

    for load in loads:
        load.wait()
    for swap in swaps:
        swap.wait_recv()
    expert(0)
    forward(nz - 1)
    expert(1)
    early_x = go(send(pb.at[1], rxb, esend.at[0], erecv.at[0], xn))
    expert(2)
    early_y = go(send(pa.at[2], rya, esend.at[1], erecv.at[1], yn))
    for d in range(nz):
        fx[d].wait_recv()
        fy[d].wait_recv()
    expert(3)
    order = list(range(1, nz)) + [0]
    dx, dy, cx, cy, zq = {}, {}, {}, {}, {}
    for d in order:
        dy[d] = go(send(pa.at[3, at(d)], da.at[at(d)], dsend.at[0, d], drecv.at[0, d], yn))
        dx[d] = go(send(pb.at[3, at(d)], db.at[at(d)], dsend.at[1, d], drecv.at[1, d], xn))
    f32 = jnp.float32
    for d in order:
        dy[d].wait_recv()
        pa[1, at(d)] = (pa[1, at(d)].astype(f32) + da[at(d)].astype(f32)).astype(jnp.bfloat16)
        cx[d] = go(send(pa.at[1, at(d)], rxa.at[at(d)], csend.at[0, d], crecv.at[0, d], xn))
        dx[d].wait_recv()
        pb[2, at(d)] = (pb[2, at(d)].astype(f32) + db[at(d)].astype(f32)).astype(jnp.bfloat16)
        cy[d] = go(send(pb.at[2, at(d)], ryb.at[at(d)], csend.at[1, d], crecv.at[1, d], yn))
    early_x.wait_recv()
    early_y.wait_recv()
    for d in order:
        cx[d].wait_recv()
        cy[d].wait_recv()
        sums = []
        for p, u, v in ((pa, rxa, rya), (pb, rxb, ryb)):
            sums.append(p[0, at(d)].astype(f32) + u[at(d)].astype(f32) + v[at(d)].astype(f32))
        if d:
            zs[d - 1, :, 0:half] = sums[0].astype(jnp.bfloat16)
            zs[d - 1, :, half:width] = sums[1].astype(jnp.bfloat16)
            zq[d] = go(send(zs.at[d - 1], rz.at[d - 1], qsend.at[d - 1], qrecv.at[d - 1], zn(at(d))))
        else:
            own[:, 0:half] = sums[0]
            own[:, half:width] = sums[1]
    total = own[...]
    for d in range(1, nz):
        zq[d].wait_recv()
        total += rz[d - 1].astype(f32)
    total = total.astype(jnp.bfloat16)
    fin[0] = total[:, 0:half]
    fin[1] = total[:, half:width]
    swap = go(send(fin.at[1 - core], rfin, fsend, frecv, other))
    out_ref[pl.ds(core * rows, rows), :] = fin[core]
    swap.wait_recv()
    out_ref[pl.ds((1 - core) * rows, rows), :] = rfin[...]
    for copy in sent:
        copy.wait_send()


def multicast(tokens, gate_weights, expert_ids, w_gate, w_up, w_down):
    tok_dev, half = tokens.shape
    nz = lax.axis_size("ep") // 4
    rows, width, ff = tok_dev // 2, w_gate.shape[1], w_gate.shape[2]
    bf, dma = jnp.bfloat16, pltpu.SemaphoreType.DMA
    vmem, hbm = pl.BlockSpec(memory_space=pltpu.VMEM), pl.BlockSpec(memory_space=pl.ANY)
    return pl.pallas_call(
        functools.partial(kernel, nz),
        out_shape=jax.ShapeDtypeStruct((tok_dev, half), bf),
        in_specs=[vmem, vmem, vmem, hbm, hbm, hbm],
        out_specs=vmem,
        scratch_shapes=[
            pltpu.VMEM((4, nz, rows, width + 128), bf),
            pltpu.VMEM((2, width, 2 * ff), bf),
            pltpu.VMEM((2 * ff, width), bf),
            pltpu.VMEM((4, nz, rows, half), bf),
            pltpu.VMEM((4, nz, rows, half), bf),
            pltpu.VMEM((nz, rows, half), bf),
            pltpu.VMEM((nz, rows, half), bf),
            pltpu.VMEM((nz, rows, half), bf),
            pltpu.VMEM((nz, rows, half), bf),
            pltpu.VMEM((nz, rows, half), bf),
            pltpu.VMEM((nz, rows, half), bf),
            pltpu.VMEM((rows, width), jnp.float32),
            pltpu.VMEM((nz - 1, rows, width), bf),
            pltpu.VMEM((nz - 1, rows, width), bf),
            pltpu.VMEM((2, rows, half), bf),
            pltpu.VMEM((rows, half), bf),
            dma((4,)), dma((2,)), dma((3,)), dma((3,)),
            dma((nz - 1,)), dma((nz - 1,)),
            dma((nz,)), dma((nz,)), dma((nz,)), dma((nz,)),
            dma((nz,)), dma((nz,)), dma((nz,)), dma((nz,)),
            dma((2,)), dma((2,)), dma((2, nz)), dma((2, nz)), dma((2, nz)), dma((2, nz)),
            dma((nz - 1,)), dma((nz - 1,)), dma, dma,
        ],
        compiler_params=pltpu.CompilerParams(
            collective_id=0, has_side_effects=True, vmem_limit_bytes=60 * 1024 * 1024
        ),
    )(tokens, gate_weights, expert_ids, w_gate, w_up, w_down)


def local(tokens, gate_weights, expert_ids, w_gate, w_up, w_down):
    tok_dev, half = tokens.shape
    devices, cores = lax.axis_size("ep"), lax.axis_size("half")
    experts = w_gate.shape[0] * devices
    gathered = tok_dev * devices * half * 2
    fits = gathered <= 8 * 1024 * 1024 and experts <= 64 and w_gate.shape[0] == 1
    shaped = cores == 2 and devices % 4 == 0 and devices > 4 and tok_dev % 32 == 0
    plan = multicast if fits and shaped else slots
    return plan(tokens, gate_weights, expert_ids, w_gate, w_up, w_down)


def solution(mesh):
    placed = (
        P("ep", "half"),
        P("ep", None),
        P("ep", None),
        P("ep", None, "half"),
        P("ep", None, "half"),
        P("ep", "half", None),
    )
    return jax.shard_map(
        local, mesh=mesh, in_specs=placed, out_specs=P("ep", "half"), check_vma=False
    )
```

```python
import functools

import jax
import jax.numpy as jnp
from jax import lax
from jax.experimental import pallas as pl
from jax.experimental.pallas import tpu as pltpu
from jax.sharding import PartitionSpec as P

MESH = pl.DeviceIdType.MESH


def slots(tokens, gate_weights, expert_ids, w_gate, w_up, w_down):
    tok_dev, half_width = tokens.shape
    top = expert_ids.shape[1]
    local_experts = w_gate.shape[0]
    experts = local_experts * lax.axis_size("ep")
    capacity = min(tok_dev, max(2, 5 * tok_dev * top // (4 * experts)))
    flat_ids = expert_ids.reshape(-1)
    columns = jnp.arange(experts, dtype=jnp.int32)
    onehot = (flat_ids[:, None] == columns[None, :]).astype(jnp.int32)
    ranks = jnp.sum((jnp.cumsum(onehot, axis=0) - onehot) * onehot, axis=1)
    slot = flat_ids * capacity + ranks
    token_of_pair = jnp.arange(tok_dev * top, dtype=jnp.int32) // top
    token_table = jnp.zeros((experts * capacity,), jnp.int32).at[slot].set(token_of_pair)
    filled = (
        jnp.zeros((experts * capacity,), jnp.bfloat16)
        .at[slot]
        .set(jnp.ones((tok_dev * top,), jnp.bfloat16))
    )
    outgoing = (tokens[token_table] * filled[:, None]).reshape(experts, capacity, half_width)
    received = lax.all_to_all(outgoing, "ep", split_axis=0, concat_axis=0, tiled=True)
    count = received.shape[1]
    whole = lax.all_gather(received, "half", axis=2, tiled=True)
    width = whole.shape[2]
    grouped = whole.reshape(-1, local_experts, count, width)
    gate = jnp.einsum("secd,edf->secf", grouped, w_gate, preferred_element_type=jnp.float32)
    up = jnp.einsum("secd,edf->secf", grouped, w_up, preferred_element_type=jnp.float32)
    hidden = (jax.nn.silu(gate) * up).astype(jnp.bfloat16)
    partial_out = jnp.einsum("secf,efd->secd", hidden, w_down, preferred_element_type=jnp.float32)
    partial_out = partial_out.astype(jnp.bfloat16).reshape(experts, count, width)
    widened = lax.optimization_barrier(partial_out).astype(jnp.float32)
    summed = lax.psum_scatter(widened.astype(jnp.bfloat16), "half", scatter_dimension=2, tiled=True)
    answer = lax.all_to_all(summed, "ep", split_axis=0, concat_axis=0, tiled=True)
    picked = answer.reshape(experts * capacity, -1)[slot].reshape(tok_dev, top, -1)
    slot_out = picked.astype(jnp.float32)
    mixed = jnp.einsum("tk,tkx->tx", gate_weights, slot_out)
    return mixed.astype(jnp.bfloat16)


def kernel(nz, tok_ref, gw_ref, ids_ref, wg_ref, wu_ref, wd_ref, out_ref,
           xg, wgu, wdn, pa, pb, da, db, rxa, rxb, rya, ryb, own, zs, rz, fin, rfin,
           load_sem, pre_sem, wsend, wrecv, zsend, zrecv, xsend, xrecv, ysend, yrecv,
           fxsend, fxrecv, fysend, fyrecv,
           esend, erecv, dsend, drecv, csend, crecv, qsend, qrecv, fsend, frecv):
    ep = lax.axis_index("ep")
    core = lax.axis_index("half")
    x, y, z = ep % 2, (ep // 2) % 2, ep // 4
    rows, width = out_ref.shape[0] // 2, wg_ref.shape[1]
    half, ff = width // 2, wg_ref.shape[2]
    other = {"half": 1 - core}
    xn = {"ep": z * 4 + y * 2 + (1 - x)}
    yn = {"ep": z * 4 + (1 - y) * 2 + x}

    def zn(to):
        return {"ep": to * 4 + y * 2 + x}

    def send(src, dst, s, r, to):
        return pltpu.make_async_remote_copy(
            src_ref=src, dst_ref=dst, send_sem=s, recv_sem=r, device_id=to, device_id_type=MESH
        )

    def at(d):
        bit, to = 1, z
        while bit < nz:
            if d & bit:
                to = to + bit - 2 * bit * ((z // bit) % 2)
            bit *= 2
        return to

    loads = [
        pltpu.make_async_copy(wg_ref.at[0], wgu.at[0, :, pl.ds(0, ff)], load_sem.at[0]),
        pltpu.make_async_copy(wu_ref.at[0], wgu.at[0, :, pl.ds(ff, ff)], load_sem.at[1]),
        pltpu.make_async_copy(wd_ref.at[0], wdn.at[pl.ds(0, ff)], load_sem.at[2]),
    ]
    mine = pltpu.make_async_copy(
        tok_ref.at[pl.ds(core * rows, rows)],
        xg.at[0, z, :, pl.ds(pl.multiple_of(core * half, 128), half)],
        load_sem.at[3],
    )
    mine.start()
    for load in loads:
        load.start()

    expert_at = lax.broadcasted_iota(jnp.int32, (128, 2 * rows), 0) % 64
    spread = jnp.zeros((128, 2 * rows), jnp.float32)
    for k in range(ids_ref.shape[0]):
        spread += jnp.where(expert_at == ids_ref[k : k + 1, :], gw_ref[k : k + 1, :], 0.0)
    spread = jnp.transpose(spread)
    spread = jnp.where(core == 0, spread[:rows], spread[rows:])
    lane = lax.broadcasted_iota(jnp.int32, (rows, 128), 1)
    upper = spread.astype(jnp.bfloat16).astype(jnp.float32)
    both = jnp.where(lane < 64, upper, spread - upper)
    xg[0, z, :, width : width + 128] = both.astype(jnp.bfloat16)

    barrier = pltpu.get_barrier_semaphore()
    partners = [other, xn, yn] + [zn(at(d)) for d in range(1, nz)]
    for partner in partners:
        pl.semaphore_signal(barrier, inc=1, device_id=partner, device_id_type=MESH)
    pl.semaphore_wait(barrier, len(partners))

    pre = send(
        tok_ref.at[pl.ds((1 - core) * rows, rows)],
        xg.at[0, z, :, pl.ds(pl.multiple_of(core * half, 128), half)],
        pre_sem.at[0], pre_sem.at[1], other,
    )
    pre.start()
    swaps = [
        send(wg_ref.at[0], wgu.at[1, :, pl.ds(0, ff)], wsend.at[0], wrecv.at[0], other),
        send(wu_ref.at[0], wgu.at[1, :, pl.ds(ff, ff)], wsend.at[1], wrecv.at[1], other),
        send(wd_ref.at[0], wdn.at[pl.ds(ff, ff)], wsend.at[2], wrecv.at[2], other),
    ]
    mine.wait()
    pre.wait_recv()
    sent = [pre]

    def go(copy):
        copy.start()
        sent.append(copy)
        return copy

    first, last = pl.ds(0, half), pl.ds(half, half + 128)
    xs, ys, fx, fy, zc = {}, {}, {}, {}, {}

    def column(d):
        b = xg.at[0, at(d)]
        for p, cols in enumerate((first, last)):
            xs[d, p] = go(send(b.at[:, cols], xg.at[1, at(d), :, cols],
                               xsend.at[p, d], xrecv.at[p, d], xn))
        for p, cols in ((1, last), (0, first)):
            ys[d, p] = go(send(b.at[:, cols], xg.at[2, at(d), :, cols],
                               ysend.at[p, d], yrecv.at[p, d], yn))

    def forward(d):
        ys[d, 1].wait_recv()
        fx[d] = go(send(xg.at[2, at(d), :, last], xg.at[3, at(d), :, last],
                        fxsend.at[d], fxrecv.at[d], xn))
        xs[d, 0].wait_recv()
        fy[d] = go(send(xg.at[1, at(d), :, first], xg.at[3, at(d), :, first],
                        fysend.at[d], fyrecv.at[d], yn))

    hops = sorted(range(1, nz), key=lambda d: bin(d ^ (d >> 1)).count("1"))
    for d in hops:
        zc[d] = go(send(xg.at[0, z], xg.at[0, z], zsend.at[d - 1], zrecv.at[d - 1], zn(at(d))))
    column(0)
    for swap in swaps:
        go(swap)
    forward(0)
    for place, d in enumerate(hops):
        zc[d].wait_recv()
        column(d)
        if place:
            forward(hops[place - 1])

    many = nz * rows

    def expert(g):
        lanes = lax.broadcasted_iota(jnp.int32, (many, 128), 1)
        table = xg[g, :, :, width : width + 128].reshape(many, 128).astype(jnp.float32)
        weight = jnp.sum(jnp.where(lanes % 64 == ep, table, 0.0), axis=1, keepdims=True)
        rows_in = xg[g, :, :, 0:width].reshape(many, width)
        parts = []
        for side in range(2):
            gu = jnp.dot(rows_in, wgu[side], preferred_element_type=jnp.float32)
            gate, up = gu[:, :ff], gu[:, ff:]
            hid = gate / (1.0 + jnp.exp(-gate)) * up * weight
            parts.append(hid.astype(jnp.bfloat16))
        hidden = jnp.concatenate(parts, axis=1)
        for to, start in ((pa, 0), (pb, half)):
            o = jnp.dot(hidden, wdn[:, start : start + half], preferred_element_type=jnp.float32)
            to[g] = o.astype(jnp.bfloat16).reshape(nz, rows, half)

    for load in loads:
        load.wait()
    for swap in swaps:
        swap.wait_recv()
    expert(0)
    forward(hops[-1])
    for d in range(nz):
        xs[d, 1].wait_recv()
    expert(1)
    early_x = go(send(pb.at[1], rxb, esend.at[0], erecv.at[0], xn))
    for d in range(nz):
        ys[d, 0].wait_recv()
    expert(2)
    early_y = go(send(pa.at[2], rya, esend.at[1], erecv.at[1], yn))
    for d in range(nz):
        fx[d].wait_recv()
        fy[d].wait_recv()
    expert(3)
    order = hops[::-1] + [0]
    dx, dy, cx, cy, zq = {}, {}, {}, {}, {}
    f32 = jnp.float32

    def corner(d):
        dy[d] = go(send(pa.at[3, at(d)], da.at[at(d)], dsend.at[0, d], drecv.at[0, d], yn))
        dx[d] = go(send(pb.at[3, at(d)], db.at[at(d)], dsend.at[1, d], drecv.at[1, d], xn))

    def edge(d):
        dy[d].wait_recv()
        pa[1, at(d)] = (pa[1, at(d)].astype(f32) + da[at(d)].astype(f32)).astype(jnp.bfloat16)
        cx[d] = go(send(pa.at[1, at(d)], rxa.at[at(d)], csend.at[0, d], crecv.at[0, d], xn))
        dx[d].wait_recv()
        pb[2, at(d)] = (pb[2, at(d)].astype(f32) + db[at(d)].astype(f32)).astype(jnp.bfloat16)
        cy[d] = go(send(pb.at[2, at(d)], ryb.at[at(d)], csend.at[1, d], crecv.at[1, d], yn))

    def home(d):
        cx[d].wait_recv()
        cy[d].wait_recv()
        sums = []
        for p, u, v in ((pa, rxa, rya), (pb, rxb, ryb)):
            sums.append(p[0, at(d)].astype(f32) + u[at(d)].astype(f32) + v[at(d)].astype(f32))
        if d:
            zs[d - 1, :, 0:half] = sums[0].astype(jnp.bfloat16)
            zs[d - 1, :, half:width] = sums[1].astype(jnp.bfloat16)
            zq[d] = go(send(zs.at[d - 1], rz.at[d - 1], qsend.at[d - 1], qrecv.at[d - 1], zn(at(d))))
        else:
            own[:, 0:half] = sums[0]
            own[:, half:width] = sums[1]

    corner(order[0])
    corner(order[1])
    for place, d in enumerate(order):
        edge(d)
        if place + 2 < len(order):
            corner(order[place + 2])
        if place == 1:
            early_x.wait_recv()
            early_y.wait_recv()
        if place:
            home(order[place - 1])
    home(order[-1])
    total = own[...]
    for d in range(1, nz):
        zq[d].wait_recv()
        total += rz[d - 1].astype(f32)
    total = total.astype(jnp.bfloat16)
    fin[0] = total[:, 0:half]
    fin[1] = total[:, half:width]
    swap = go(send(fin.at[1 - core], rfin, fsend, frecv, other))
    out_ref[pl.ds(core * rows, rows), :] = fin[core]
    swap.wait_recv()
    out_ref[pl.ds((1 - core) * rows, rows), :] = rfin[...]
    for copy in sent:
        copy.wait_send()


def multicast(tokens, gate_weights, expert_ids, w_gate, w_up, w_down):
    tok_dev, half = tokens.shape
    nz = lax.axis_size("ep") // 4
    rows, width, ff = tok_dev // 2, w_gate.shape[1], w_gate.shape[2]
    bf, dma = jnp.bfloat16, pltpu.SemaphoreType.DMA
    vmem, hbm = pl.BlockSpec(memory_space=pltpu.VMEM), pl.BlockSpec(memory_space=pl.ANY)
    return pl.pallas_call(
        functools.partial(kernel, nz),
        out_shape=jax.ShapeDtypeStruct((tok_dev, half), bf),
        in_specs=[vmem, vmem, vmem, hbm, hbm, hbm],
        out_specs=vmem,
        scratch_shapes=[
            pltpu.VMEM((4, nz, rows, width + 128), bf),
            pltpu.VMEM((2, width, 2 * ff), bf),
            pltpu.VMEM((2 * ff, width), bf),
            pltpu.VMEM((4, nz, rows, half), bf),
            pltpu.VMEM((4, nz, rows, half), bf),
            pltpu.VMEM((nz, rows, half), bf),
            pltpu.VMEM((nz, rows, half), bf),
            pltpu.VMEM((nz, rows, half), bf),
            pltpu.VMEM((nz, rows, half), bf),
            pltpu.VMEM((nz, rows, half), bf),
            pltpu.VMEM((nz, rows, half), bf),
            pltpu.VMEM((rows, width), jnp.float32),
            pltpu.VMEM((nz - 1, rows, width), bf),
            pltpu.VMEM((nz - 1, rows, width), bf),
            pltpu.VMEM((2, rows, half), bf),
            pltpu.VMEM((rows, half), bf),
            dma((4,)), dma((2,)), dma((3,)), dma((3,)),
            dma((nz - 1,)), dma((nz - 1,)),
            dma((2, nz)), dma((2, nz)), dma((2, nz)), dma((2, nz)),
            dma((nz,)), dma((nz,)), dma((nz,)), dma((nz,)),
            dma((2,)), dma((2,)), dma((2, nz)), dma((2, nz)), dma((2, nz)), dma((2, nz)),
            dma((nz - 1,)), dma((nz - 1,)), dma, dma,
        ],
        compiler_params=pltpu.CompilerParams(
            collective_id=0, has_side_effects=True, vmem_limit_bytes=60 * 1024 * 1024
        ),
    )(tokens, gate_weights.T, expert_ids.T, w_gate, w_up, w_down)


def local(tokens, gate_weights, expert_ids, w_gate, w_up, w_down):
    tok_dev, half = tokens.shape
    devices, cores = lax.axis_size("ep"), lax.axis_size("half")
    experts = w_gate.shape[0] * devices
    gathered = tok_dev * devices * half * 2
    fits = gathered <= 8 * 1024 * 1024 and experts <= 64 and w_gate.shape[0] == 1
    shaped = cores == 2 and devices % 4 == 0 and devices > 4 and devices & (devices - 1) == 0 and tok_dev % 32 == 0
    plan = multicast if fits and shaped else slots
    return plan(tokens, gate_weights, expert_ids, w_gate, w_up, w_down)


def solution(mesh):
    placed = (
        P("ep", "half"),
        P("ep", None),
        P("ep", None),
        P("ep", None, "half"),
        P("ep", None, "half"),
        P("ep", "half", None),
    )
    return jax.shard_map(
        local, mesh=mesh, in_specs=placed, out_specs=P("ep", "half"), check_vma=False
    )
```
